32 devices in a mesh: row: 8 (over z, core), col: 4 (over y, x).
Axes of the slice: x: 2, y: 2, z: 4, core: 2. Of those that a mesh axis runs over, the one named last changes fastest.
Arguments:
- train_weight: bfloat16 [4, 4608, 2048], P(None, 'row', 'col')
- src_map: int32 [16], replicated, may hold values from 0 to 15, as said below
- tgt_map: int32 [16], replicated, may hold values from 0 to 15, as said below
- probe: bfloat16 [4096, 4608], P('row'), may hold values from -6 to 6
Outputs:
- codes: bfloat16 [4, 4608, 2048], P(None, None, 'col')
- peaks: float32 [4, 16], P(None, 'col')
- checked: bfloat16 [4, 4096, 2048], P(None, 'row', 'col')
The draws below stay inside these ranges and needn't reach their ends.
Inputs may be any that keep to these rules, and one draw needn't show every extreme that they name: src_map is a permutation of 0 to 15. tgt_map is a permutation of 0 to 15. Call column k the slots k * 4 to (k + 1) * 4 - 1 of a map, and let C = 4. There are three different offsets a, b, c in 0 to C - 1, the same for every column, of which one is C / 2 and one is C - 1: the heads of training column k stand in serving columns (k - a) mod C (2 of them), (k - b) mod C (one) and (k - c) mod C (one).
All inputs are finite; a program needn't handle non-finite values. Where the reference program divides by a largest or mean magnitude, that divisor is 1e-20 or more.
Results may differ from the reference program's by a relative error of at most 0.0049.
Values may be sent and summed in bfloat16 or wider, within the bound.
A program may use at most 128 MiB of HBM per device.

```python
import jax
import jax.numpy as jnp

D = 4608
HDIM = 128
HCOL = 4
LAYERS = 4
TOKENS = 4096
N_COL = 4


def head_maps(key):
    heads_all = HCOL * N_COL
    keys = jax.random.split(jax.random.fold_in(key, 17), 6)
    source = jax.random.permutation(keys[0], heads_all).astype(jnp.int32)
    half = N_COL // 2
    before_one = jnp.array([N_COL - 1], jnp.int32)
    picked = jax.random.randint(keys[5], (1,), 0, N_COL - 2).astype(jnp.int32)
    third = jnp.where(picked < half, picked, picked + 1).astype(jnp.int32)
    three = jnp.concatenate([jnp.array([half], jnp.int32), before_one, third])
    offsets = three[jax.random.permutation(keys[4], 3)].astype(jnp.int32)
    pattern = jnp.array([0, 0, 1, 2], jnp.int32)
    roles = jax.vmap(lambda single: jax.random.permutation(single, 4))(jax.random.split(keys[2], N_COL)).astype(jnp.int32)
    locals_order = jax.vmap(lambda single: jax.random.permutation(single, 4))(jax.random.split(keys[3], N_COL)).astype(jnp.int32)
    targets = jnp.arange(N_COL, dtype=jnp.int32)[:, None]
    shifted = offsets[pattern[roles]]
    from_col = (targets + shifted) % N_COL
    local_slot = locals_order[from_col, roles]
    target = source[(from_col * HCOL + local_slot).reshape(-1)]
    return (source, target.astype(jnp.int32))


def draw_src_map(key, part):
    return head_maps(key)[0]


def draw_tgt_map(key, part):
    return head_maps(key)[1]


def draw_train_weight(key, part):
    keys = jax.random.split(jax.random.fold_in(key, 5), 3)
    heads_all = HCOL * N_COL
    head_scale = jnp.exp(jax.random.uniform(keys[1], (LAYERS, 1, heads_all, 1), jnp.float32, jnp.log(0.3), jnp.log(3.0)))
    row_scale = jnp.exp(jax.random.uniform(keys[2], (1, D, 1, 1), jnp.float32, jnp.log(0.4), jnp.log(4.0)))
    base = jax.random.normal(keys[0], (LAYERS, D, heads_all, HDIM), jnp.float32)
    weights = base * head_scale * row_scale / jnp.sqrt(jnp.float32(D))
    return weights.reshape(LAYERS, D, heads_all * HDIM).astype(jnp.bfloat16)


def block_scale(stream_key, shape, cuts, smallest, high):
    def one(position, shards_of):
        heights = jax.random.uniform(jax.random.fold_in(jax.random.fold_in(stream_key, 6), position), (shards_of,), jnp.float32, smallest / len(cuts), high / len(cuts))
        return jnp.repeat(jnp.exp(heights), shape[position] // shards_of).reshape((-1,) + (1,) * (len(shape) - position - 1))

    loudness = one(*cuts[0])
    for cut in cuts[1:]:
        loudness = loudness * one(*cut)
    return loudness


def bell_draw(stream_key, shape, spread, most, cuts=(), kind=jnp.bfloat16):
    loudness = block_scale(stream_key, shape, cuts, -0.22, 0.18) if cuts else 1.0
    entries = jax.random.normal(stream_key, shape, jnp.float32) * spread * loudness
    return jnp.minimum(jnp.maximum(entries, -most), most).astype(kind)


def setup_inputs(seed: int = 0) -> dict:
    streams_of = jax.random.split(jax.random.key(seed), 5)
    return {
        "train_weight": draw_train_weight(jax.random.fold_in(streams_of[4], 71), 0),
        "src_map": draw_src_map(jax.random.fold_in(streams_of[4], 71), 0),
        "tgt_map": draw_tgt_map(jax.random.fold_in(streams_of[4], 71), 0),
        "probe": bell_draw(streams_of[3], (TOKENS, D), 1.0, 6.0, ((0, 8),)),
    }


def reference(train_weight, src_map, tgt_map, probe):
    heads_all = src_map.shape[0]
    slot_ids = jnp.arange(heads_all, dtype=jnp.int32)
    matched = (src_map[None, :] == tgt_map[:, None]).astype(jnp.int32)
    source = jnp.sum(matched * slot_ids[None, :], axis=1).astype(jnp.int32)
    heads_four = train_weight.reshape(LAYERS, D, heads_all, HDIM)
    served = jnp.take(heads_four, source, axis=2)
    peaks = jnp.max(jnp.abs(served.astype(jnp.float32)), axis=(1, 3))
    codes = (served.astype(jnp.float32) / (peaks[:, None, :, None] + 1e-6)).astype(jnp.bfloat16)
    codes = codes.reshape(LAYERS, D, heads_all * HDIM)
    results = []
    for layer in range(LAYERS):
        projected = jnp.dot(probe, codes[layer], preferred_element_type=jnp.float32)
        scaled = projected * jnp.repeat(peaks[layer], HDIM)[None, :]
        results.append(scaled.astype(jnp.bfloat16))
    return codes, peaks, jnp.stack(results)
```

```python
import functools

import jax
import jax.numpy as jnp
from jax import lax
from jax.experimental import pallas as pl
from jax.experimental.pallas import tpu as pltpu
from jax.sharding import PartitionSpec as P

HDIM = 128
CORES = 2
TILE = 16
KSTEP = 512
MESH = pl.DeviceIdType.MESH


def pieces_of(rows, most):
    for count in range(most, 0, -1):
        if rows % (TILE * count) == 0:
            return count
    return 1


def chunk_list(layers, rows):
    out = []
    for layer in range(layers):
        count = pieces_of(rows, 4 if layer == 0 else 2)
        size = rows // count
        for i in range(count):
            out.append((layer, i * size, size))
    return out


def kernel(
    chunks, zs, cols, source_ref, w_ref, probe_ref, codes_ref, checked_ref, peaks_ref,
    full, cbuf, pbuf, chk, guard,
    csend, crecv, zsend, zrecv, local, outsem, *raws,
):
    layers, heads, width, _ = full.shape
    rows = w_ref.shape[1]
    tokens = pbuf.shape[0]
    me = lax.axis_index("row")
    mycol = lax.axis_index("col")
    z = me // CORES
    core = me % CORES
    partner = z * CORES + (1 - core)
    has_down = z > 0
    has_up = z < zs - 1

    barrier = pltpu.get_barrier_semaphore()
    for o in range(1, cols):
        pl.semaphore_signal(
            barrier, inc=1, device_id={"col": lax.rem(mycol + o, cols)}, device_id_type=MESH
        )
    pl.semaphore_signal(barrier, inc=1, device_id={"row": partner}, device_id_type=MESH)

    @pl.when(has_down)
    def _():
        pl.semaphore_signal(barrier, inc=1, device_id={"row": me - CORES}, device_id_type=MESH)

    @pl.when(has_up)
    def _():
        pl.semaphore_signal(barrier, inc=1, device_id={"row": me + CORES}, device_id_type=MESH)

    pl.semaphore_wait(barrier, cols + has_down.astype(jnp.int32) + has_up.astype(jnp.int32))

    def raw_at(g, owner, head):
        return raws[g].at[owner * heads + head]

    def col_copy(g, owner, target, head):
        layer, r0, size = chunks[g]
        return pltpu.make_async_remote_copy(
            src_ref=w_ref.at[layer, pl.ds(r0, size), pl.ds(head * HDIM, HDIM)],
            dst_ref=raw_at(g, owner, head),
            send_sem=csend.at[g, target, head],
            recv_sem=crecv.at[g, owner, head],
            device_id={"col": target},
            device_id_type=MESH,
        )

    def own_copy(g, head):
        layer, r0, size = chunks[g]
        return pltpu.make_async_copy(
            w_ref.at[layer, pl.ds(r0, size), pl.ds(head * HDIM, HDIM)],
            raw_at(g, mycol, head),
            local.at[g, head],
        )

    for g in range(len(chunks)):
        for head in range(heads):
            for o in range(1, cols):
                col_copy(g, mycol, lax.rem(mycol + o, cols), head).start()
            own_copy(g, head).start()
    probe_copy = pltpu.make_async_copy(probe_ref, pbuf, outsem.at[0])
    probe_copy.start()

    def row_copy(g, zb, cb, way, target):
        layer, r0, size = chunks[g]
        block = zb * CORES + cb
        ref = full.at[layer, :, pl.ds(pl.multiple_of(block * rows + r0, TILE), size), :]
        return pltpu.make_async_remote_copy(
            src_ref=ref,
            dst_ref=ref,
            send_sem=zsend.at[g, zb, way],
            recv_sem=zrecv.at[g, block],
            device_id={"row": target},
            device_id_type=MESH,
        )

    down, up = me - CORES, me + CORES

    def stage_own(g):
        layer, r0, size = chunks[g]
        for head in range(heads):
            for o in range(1, cols):
                col_copy(g, lax.rem(mycol + o, cols), mycol, head).wait_recv()
            own_copy(g, head).wait()
        start = pl.multiple_of(me * rows + r0, TILE)

        @pl.loop(0, heads)
        def _(t):
            full[layer, t, pl.ds(start, size), :] = raws[g][source_ref[t]]

        @pl.loop(0, heads)
        def _(t):
            block = full[layer, t, pl.ds(start, size), :]
            guard[t] = jnp.max(block.reshape(-1, TILE, HDIM), axis=0)

        @pl.when(has_down)
        def _():
            row_copy(g, z, core, 0, down).start()

        @pl.when(has_up)
        def _():
            row_copy(g, z, core, 1, up).start()

        row_copy(g, z, core, 2, partner).start()

    def stage_forward(g):
        for h in range(1, zs):
            @pl.when(z + h < zs)
            def _():
                row_copy(g, z + h, core, 0, down).wait_recv()

                @pl.when(has_down)
                def _():
                    row_copy(g, z + h, core, 0, down).start()

                row_copy(g, z + h, core, 2, partner).start()

            @pl.when(z - h >= 0)
            def _():
                row_copy(g, z - h, core, 1, up).wait_recv()

                @pl.when(has_up)
                def _():
                    row_copy(g, z - h, core, 1, up).start()

                row_copy(g, z - h, core, 2, partner).start()

    def codes_copy(layer):
        return pltpu.make_async_copy(
            cbuf.at[layer % 2], codes_ref.at[layer], outsem.at[1 + layer % 2]
        )

    def checked_copy(layer):
        return pltpu.make_async_copy(
            chk.at[layer % 2], checked_ref.at[layer], outsem.at[3 + layer % 2]
        )

    def compute(layer):
        for g, chunk in enumerate(chunks):
            if chunk[0] == layer:
                @pl.loop(0, zs)
                def _(zb):
                    row_copy(g, zb, 1 - core, 2, partner).wait_recv()
        if layer == 0:
            probe_copy.wait()
        if layer >= 2:
            codes_copy(layer - 2).wait()
            checked_copy(layer - 2).wait()
        slot = layer % 2

        def most(i, acc):
            at = pl.ds(pl.multiple_of(i * KSTEP, KSTEP), KSTEP)
            return tuple(
                jnp.maximum(
                    acc[t],
                    jnp.max(jnp.abs(full[layer, t, at, :]).reshape(-1, TILE, HDIM), axis=0),
                )
                for t in range(heads)
            )

        zero = jnp.zeros((TILE, HDIM), full.dtype)
        best = lax.fori_loop(0, width // KSTEP, most, (zero,) * heads)
        tops = [
            jnp.max(jnp.max(b.astype(jnp.float32), axis=0, keepdims=True), axis=1, keepdims=True)
            for b in best
        ]
        spread = [jnp.broadcast_to(p, (1, HDIM)) for p in tops]
        inverse = [1.0 / ((p + 1e-06) * 0.25) for p in spread]
        here = lax.broadcasted_iota(jnp.int32, peaks_ref.shape, 0) == layer
        lane = lax.broadcasted_iota(jnp.int32, peaks_ref.shape, 1)
        for t in range(heads):
            peaks_ref[...] = jnp.where(here & (lane == t), tops[t], peaks_ref[...])
        for t0 in range(0, heads, 2):
            def step(i, acc):
                at = pl.ds(pl.multiple_of(i * KSTEP, KSTEP), KSTEP)
                both = jnp.concatenate(
                    [
                        (
                            (full[layer, t, at, :].astype(jnp.float32) * 0.25) * inverse[t]
                        ).astype(cbuf.dtype)
                        for t in (t0, t0 + 1)
                    ],
                    axis=1,
                )
                cbuf[slot, at, pl.ds(t0 * HDIM, 2 * HDIM)] = both
                return acc + jnp.dot(pbuf[:, at], both, preferred_element_type=jnp.float32)

            acc = lax.fori_loop(
                0, width // KSTEP, step, jnp.zeros((tokens, 2 * HDIM), jnp.float32)
            )
            scale = jnp.concatenate([spread[t0], spread[t0 + 1]], axis=1)
            chk[slot, :, pl.ds(t0 * HDIM, 2 * HDIM)] = (acc * scale).astype(chk.dtype)
        codes_copy(layer).start()
        checked_copy(layer).start()

    peaks_ref[...] = jnp.zeros_like(peaks_ref)
    total = len(chunks)
    stage_own(0)
    stage_own(1)
    for g in range(total):
        stage_forward(g)
        if g + 2 < total:
            stage_own(g + 2)
        if g + 1 == total or chunks[g + 1][0] != chunks[g][0]:
            compute(chunks[g][0])

    for layer in range(max(layers - 2, 0), layers):
        codes_copy(layer).wait()
        checked_copy(layer).wait()
    for g in range(total):
        for o in range(1, cols):
            for head in range(heads):
                col_copy(g, mycol, lax.rem(mycol + o, cols), head).wait_send()

        @pl.loop(0, zs)
        def _(zb):
            @pl.when(has_down & (zb >= z))
            def _():
                row_copy(g, zb, core, 0, down).wait_send()

            @pl.when(has_up & (zb <= z))
            def _():
                row_copy(g, zb, core, 1, up).wait_send()

            row_copy(g, zb, core, 2, partner).wait_send()


def per_device(train_weight, src_map, tgt_map, probe):
    cols = lax.axis_size("col")
    count = lax.axis_size("row")
    per_col = src_map.shape[0] // cols
    layers, rows, span = train_weight.shape
    tokens, width = probe.shape
    zs = count // CORES
    wanted = lax.dynamic_slice(tgt_map, (lax.axis_index("col") * per_col,), (per_col,))
    source = jnp.argmax(wanted[:, None] == src_map[None, :], axis=1).astype(jnp.int32)
    chunks = chunk_list(layers, rows)
    total = len(chunks)
    anywhere = pl.BlockSpec(memory_space=pl.ANY)
    smem = pl.BlockSpec(memory_space=pltpu.SMEM)
    dtype = train_weight.dtype
    codes, checked, peaks = pl.pallas_call(
        functools.partial(kernel, chunks, zs, cols),
        out_shape=(
            jax.ShapeDtypeStruct((layers, width, span), dtype),
            jax.ShapeDtypeStruct((layers, tokens, span), dtype),
            jax.ShapeDtypeStruct((layers, per_col), jnp.float32),
        ),
        in_specs=[smem, anywhere, anywhere],
        out_specs=(anywhere, anywhere, pl.BlockSpec(memory_space=pltpu.VMEM)),
        scratch_shapes=[
            pltpu.VMEM((layers, per_col, width, HDIM), dtype),
            pltpu.VMEM((2, width, span), dtype),
            pltpu.VMEM((tokens, width), dtype),
            pltpu.VMEM((2, tokens, span), dtype),
            pltpu.VMEM((per_col, TILE, HDIM), dtype),
            pltpu.SemaphoreType.DMA((total, cols, per_col)),
            pltpu.SemaphoreType.DMA((total, cols, per_col)),
            pltpu.SemaphoreType.DMA((total, zs, 3)),
            pltpu.SemaphoreType.DMA((total, count)),
            pltpu.SemaphoreType.DMA((total, per_col)),
            pltpu.SemaphoreType.DMA((5,)),
        ]
        + [pltpu.VMEM((cols * per_col, size, HDIM), dtype) for _, _, size in chunks],
        compiler_params=pltpu.CompilerParams(
            collective_id=0, has_side_effects=True, vmem_limit_bytes=67043328
        ),
    )(source, train_weight, probe)
    return codes, peaks, checked


def solution(mesh):
    in_specs = (P(None, "row", "col"), P(), P(), P("row", None))
    out_specs = (P(None, None, "col"), P(None, "col"), P(None, "row", "col"))
    return jax.shard_map(
        per_device, mesh=mesh, in_specs=in_specs, out_specs=out_specs, check_vma=False
    )
```

```python
import functools

import jax
import jax.numpy as jnp
from jax import lax
from jax.experimental import pallas as pl
from jax.experimental.pallas import tpu as pltpu
from jax.sharding import PartitionSpec as P

HDIM = 128
CORES = 2
TILE = 16
KSTEP = 512
MESH = pl.DeviceIdType.MESH


def pieces_of(rows, most):
    for count in range(most, 0, -1):
        if rows % (TILE * count) == 0:
            return count
    return 1


def piece_list(layers, rows):
    out = []
    for layer in range(layers):
        count = pieces_of(rows, 4 if layer == 0 else (1 if layer == layers - 1 else 2))
        size = rows // count
        for i in range(count):
            out.append((layer, i * size, size))
    return out


def chunk_list(pieces, layers, heads):
    out = []
    for e, (layer, _, _) in enumerate(pieces):
        step = 2 if layer == layers - 1 else heads
        out.extend((e, h0, step) for h0 in range(0, heads, step))
    return out


def kernel(
    pieces, chunks, zs, cols, source_ref, w_ref, probe_ref, codes_ref, checked_ref, peaks_ref,
    full, pbuf, guard,
    csend, crecv, zsend, zrecv, local, probesem, *raws,
):
    layers, heads, width, _ = full.shape
    rows = w_ref.shape[1]
    tokens = pbuf.shape[0]
    me = lax.axis_index("row")
    mycol = lax.axis_index("col")
    z = me // CORES
    core = me % CORES
    partner = z * CORES + (1 - core)
    has_down = z > 0
    has_up = z < zs - 1

    barrier = pltpu.get_barrier_semaphore()
    for o in range(1, cols):
        pl.semaphore_signal(
            barrier, inc=1, device_id={"col": lax.rem(mycol + o, cols)}, device_id_type=MESH
        )
    pl.semaphore_signal(barrier, inc=1, device_id={"row": partner}, device_id_type=MESH)

    @pl.when(has_down)
    def _():
        pl.semaphore_signal(barrier, inc=1, device_id={"row": me - CORES}, device_id_type=MESH)

    @pl.when(has_up)
    def _():
        pl.semaphore_signal(barrier, inc=1, device_id={"row": me + CORES}, device_id_type=MESH)

    pl.semaphore_wait(barrier, cols + has_down.astype(jnp.int32) + has_up.astype(jnp.int32))

    def raw_at(g, owner, head):
        return raws[g].at[owner * heads + head]

    def col_copy(g, owner, target, head):
        layer, r0, size = pieces[g]
        return pltpu.make_async_remote_copy(
            src_ref=w_ref.at[layer, pl.ds(r0, size), pl.ds(head * HDIM, HDIM)],
            dst_ref=raw_at(g, owner, head),
            send_sem=csend.at[g, target, head],
            recv_sem=crecv.at[g, owner, head],
            device_id={"col": target},
            device_id_type=MESH,
        )

    def own_copy(g, head):
        layer, r0, size = pieces[g]
        return pltpu.make_async_copy(
            w_ref.at[layer, pl.ds(r0, size), pl.ds(head * HDIM, HDIM)],
            raw_at(g, mycol, head),
            local.at[g, head],
        )

    for g in range(len(pieces)):
        for head in range(heads):
            for o in range(1, cols):
                col_copy(g, mycol, lax.rem(mycol + o, cols), head).start()
            own_copy(g, head).start()
    probe_copy = pltpu.make_async_copy(probe_ref, pbuf, probesem.at[0])
    probe_copy.start()

    def row_copy(g, zb, cb, way, target):
        piece, h0, hn = chunks[g]
        layer, r0, size = pieces[piece]
        block = zb * CORES + cb
        ref = full.at[layer, pl.ds(h0, hn), pl.ds(pl.multiple_of(block * rows + r0, TILE), size), :]
        return pltpu.make_async_remote_copy(
            src_ref=ref,
            dst_ref=ref,
            send_sem=zsend.at[g, zb, way],
            recv_sem=zrecv.at[g, block],
            device_id={"row": target},
            device_id_type=MESH,
        )

    down, up = me - CORES, me + CORES

    def stage_own(g):
        piece, h0, hn = chunks[g]
        layer, r0, size = pieces[piece]
        for head in range(heads):
            if h0 == 0:
                for o in range(1, cols):
                    col_copy(piece, lax.rem(mycol + o, cols), mycol, head).wait_recv()
                own_copy(piece, head).wait()
        start = pl.multiple_of(me * rows + r0, TILE)

        @pl.loop(h0, h0 + hn)
        def _(t):
            full[layer, t, pl.ds(start, size), :] = raws[piece][source_ref[t]]

        @pl.loop(h0, h0 + hn)
        def _(t):
            block = full[layer, t, pl.ds(start, size), :]
            guard[t] = jnp.max(block.reshape(-1, TILE, HDIM), axis=0)

        @pl.when(has_down)
        def _():
            row_copy(g, z, core, 0, down).start()

        @pl.when(has_up)
        def _():
            row_copy(g, z, core, 1, up).start()

        row_copy(g, z, core, 2, partner).start()

    def stage_forward(g):
        for h in range(1, zs):
            @pl.when(z + h < zs)
            def _():
                row_copy(g, z + h, core, 0, down).wait_recv()

                @pl.when(has_down)
                def _():
                    row_copy(g, z + h, core, 0, down).start()

                row_copy(g, z + h, core, 2, partner).start()

            @pl.when(z - h >= 0)
            def _():
                row_copy(g, z - h, core, 1, up).wait_recv()

                @pl.when(has_up)
                def _():
                    row_copy(g, z - h, core, 1, up).start()

                row_copy(g, z - h, core, 2, partner).start()

    def compute(layer, t0):
        pair = (t0, t0 + 1)

        def most(i, acc):
            at = pl.ds(pl.multiple_of(i * KSTEP, KSTEP), KSTEP)
            return tuple(
                jnp.maximum(
                    acc[t - t0],
                    jnp.max(jnp.abs(full[layer, t, at, :]).reshape(-1, TILE, HDIM), axis=0),
                )
                for t in pair
            )

        zero = jnp.zeros((TILE, HDIM), full.dtype)
        best = lax.fori_loop(0, width // KSTEP, most, (zero,) * 2)
        tops = [
            jnp.max(jnp.max(b.astype(jnp.float32), axis=0, keepdims=True), axis=1, keepdims=True)
            for b in best
        ]
        spread = [jnp.broadcast_to(p, (1, HDIM)) for p in tops]
        inverse = [1.0 / ((p + 1e-06) * 0.25) for p in spread]
        here = lax.broadcasted_iota(jnp.int32, peaks_ref.shape, 0) == layer
        lane = lax.broadcasted_iota(jnp.int32, peaks_ref.shape, 1)
        for t in pair:
            peaks_ref[...] = jnp.where(here & (lane == t), tops[t - t0], peaks_ref[...])

        def step(i, acc):
            at = pl.ds(pl.multiple_of(i * KSTEP, KSTEP), KSTEP)
            both = jnp.concatenate(
                [
                    (
                        (full[layer, t, at, :].astype(jnp.float32) * 0.25) * inverse[t - t0]
                    ).astype(codes_ref.dtype)
                    for t in pair
                ],
                axis=1,
            )
            codes_ref[layer, at, pl.ds(t0 * HDIM, 2 * HDIM)] = both
            return acc + jnp.dot(pbuf[:, at], both, preferred_element_type=jnp.float32)

        acc = lax.fori_loop(0, width // KSTEP, step, jnp.zeros((tokens, 2 * HDIM), jnp.float32))
        scale = jnp.concatenate(spread, axis=1)
        checked_ref[layer, :, pl.ds(t0 * HDIM, 2 * HDIM)] = (acc * scale).astype(
            checked_ref.dtype
        )

    peaks_ref[...] = jnp.zeros_like(peaks_ref)
    total = len(chunks)
    stage_own(0)
    stage_own(1)
    for g in range(total):
        stage_forward(g)
        if g + 2 < total:
            stage_own(g + 2)
        piece, h0, hn = chunks[g]
        layer = pieces[piece][0]
        last = piece + 1 == len(pieces) or pieces[piece + 1][0] != layer
        if last:
            for k, (e, other, _) in enumerate(chunks):
                if pieces[e][0] == layer and other == h0:
                    @pl.loop(0, zs)
                    def _(zb):
                        row_copy(k, zb, 1 - core, 2, partner).wait_recv()
            if layer == 0:
                probe_copy.wait()
            for t0 in range(h0, h0 + hn, 2):
                compute(layer, t0)

    for e in range(len(pieces)):
        for o in range(1, cols):
            for head in range(heads):
                col_copy(e, mycol, lax.rem(mycol + o, cols), head).wait_send()
    for g in range(total):

        @pl.loop(0, zs)
        def _(zb):
            @pl.when(has_down & (zb >= z))
            def _():
                row_copy(g, zb, core, 0, down).wait_send()

            @pl.when(has_up & (zb <= z))
            def _():
                row_copy(g, zb, core, 1, up).wait_send()

            row_copy(g, zb, core, 2, partner).wait_send()


def per_device(train_weight, src_map, tgt_map, probe):
    cols = lax.axis_size("col")
    count = lax.axis_size("row")
    per_col = src_map.shape[0] // cols
    layers, rows, span = train_weight.shape
    tokens, width = probe.shape
    zs = count // CORES
    wanted = lax.dynamic_slice(tgt_map, (lax.axis_index("col") * per_col,), (per_col,))
    source = jnp.argmax(wanted[:, None] == src_map[None, :], axis=1).astype(jnp.int32)
    pieces = piece_list(layers, rows)
    chunks = chunk_list(pieces, layers, per_col)
    total, parts = len(chunks), len(pieces)
    grant = 2 * HDIM * (
        layers * per_col * width + per_col * layers * rows * cols
    ) + 2 * tokens * width + 2**21
    anywhere = pl.BlockSpec(memory_space=pl.ANY)
    smem = pl.BlockSpec(memory_space=pltpu.SMEM)
    dtype = train_weight.dtype
    codes, checked, peaks = pl.pallas_call(
        functools.partial(kernel, pieces, chunks, zs, cols),
        out_shape=(
            pltpu.VMEM((layers, width, span), dtype),
            pltpu.VMEM((layers, tokens, span), dtype),
            jax.ShapeDtypeStruct((layers, per_col), jnp.float32),
        ),
        in_specs=[smem, anywhere, anywhere],
        out_specs=(pl.BlockSpec(memory_space=pltpu.VMEM),) * 3,
        scratch_shapes=[
            pltpu.VMEM((layers, per_col, width, HDIM), dtype),
            pltpu.VMEM((tokens, width), dtype),
            pltpu.VMEM((per_col, TILE, HDIM), dtype),
            pltpu.SemaphoreType.DMA((parts, cols, per_col)),
            pltpu.SemaphoreType.DMA((parts, cols, per_col)),
            pltpu.SemaphoreType.DMA((total, zs, 3)),
            pltpu.SemaphoreType.DMA((total, count)),
            pltpu.SemaphoreType.DMA((parts, per_col)),
            pltpu.SemaphoreType.DMA((1,)),
        ]
        + [pltpu.VMEM((cols * per_col, size, HDIM), dtype) for _, _, size in pieces],
        compiler_params=pltpu.CompilerParams(
            collective_id=0, has_side_effects=True, vmem_limit_bytes=grant
        ),
    )(source, train_weight, probe)
    return codes, peaks, checked


def solution(mesh):
    in_specs = (P(None, "row", "col"), P(), P(), P("row", None))
    out_specs = (P(None, None, "col"), P(None, "col"), P(None, "row", "col"))
    return jax.shard_map(
        per_device, mesh=mesh, in_specs=in_specs, out_specs=out_specs, check_vma=False
    )
```
